32 devices in a mesh: cp: 16 (over z, x, core), tp: 2 (over y).
Axes of the slice: x: 2, y: 2, z: 4, core: 2. Of those that a mesh axis runs over, the one named last changes fastest.
Arguments:
- hidden: bfloat16 [8192, 4096], P('cp', 'tp'), may hold values from -6 to 6
- norm_gain: float32 [4096], replicated, may hold values from 0.5 to 1.5
- w_query: bfloat16 [4096, 4096], P(None, 'tp'), may hold values from -0.140625 to 0.140625
- w_key: bfloat16 [4096, 1024], P(None, 'tp'), may hold values from -4 to 4
- w_value: bfloat16 [4096, 1024], P(None, 'tp'), may hold values from -0.09375 to 0.09375
- w_out: bfloat16 [4096, 4096], P('tp'), may hold values from -0.5 to 0.5
- doc_ids: int32 [8192], P('cp'), may hold values from 0 to 5, never falling along the last dimension, each value on 1 to 6144 neighbouring positions
Outputs:
- updated: bfloat16 [8192, 4096], P('cp', 'tp')
The draws below stay inside these ranges and needn't reach their ends.
Inputs may be any that keep to these rules, and one draw needn't show every extreme that they name: `doc_ids`: document numbers never fall along the sequence; every document has 1 to 6144 tokens.
All inputs are finite; a program needn't handle non-finite values.
Results may differ from the reference program's by a relative error of at most 0.017.
The reference program's roundings to bfloat16 on the way count: a program that leaves them out, or rounds other values in their place, can miss the bound.
Values may be sent and summed in bfloat16 or wider, within the bound.
No kernel may reach another device: no remote copies, remote signals or barrier semaphores. Data moves between devices by JAX's collectives and lax.ppermute only.
A program may use at most 128 MiB of HBM per device.

```python
import math
import jax
import jax.numpy as jnp
import numpy as np
from jax import lax

D = 4096
HEADS = 32
KV_HEADS = 8
HEAD_SIZE = 128
TOK_DEV = 512
DOCS = 6
SEQ = 8192
LONGEST = 6144
N_TP = 2


def query_key_pair(key):
    spread = 1.5 / math.sqrt(D)
    limit = 9.0 / math.sqrt(D)
    base = jax.random.normal(jax.random.fold_in(key, 101), (D, HEADS * HEAD_SIZE), jnp.float32) * spread
    base = jnp.clip(base, -limit, limit)
    other = jax.random.normal(jax.random.fold_in(key, 202), (D, KV_HEADS * HEAD_SIZE), jnp.float32) * spread
    other = jnp.clip(other, -limit, limit)
    return (base, other)


def draw_w_query(key, part):
    base, other = query_key_pair(key)
    return base.astype(jnp.bfloat16)


def draw_w_key(key, part):
    base, other = query_key_pair(key)
    result = other
    return result.astype(jnp.bfloat16)


def block_levels(rng, dims, cuts, low, top_value):
    loudness = 1.0
    for axis_at, shards_of in cuts:
        draws = jax.random.uniform(jax.random.fold_in(jax.random.fold_in(rng, 6), axis_at), (shards_of,), jnp.float32, low / len(cuts), top_value / len(cuts))
        loudness = loudness * jnp.repeat(jnp.exp(draws), dims[axis_at] // shards_of).reshape((-1,) + (1,) * (len(dims) - 1 - axis_at))
    return loudness


def length_profile(amount, total, reach, slope):
    loads = [(1 << 20) // math.isqrt(standing ** slope) + 1 for standing in range(2, amount + 1)]
    rest, given = total - reach - (amount - 1), [1] * (amount - 1)
    while rest > 0:
        free = [i for i in range(amount - 1) if given[i] < reach]
        whole, remaining = sum([loads[i] for i in free]), rest
        for i in free:
            addition = min(reach - given[i], max(1, remaining * loads[i] // whole), rest)
            given[i] = given[i] + addition
            rest = rest - addition
    return np.array([reach] + given)


def uneven(own_key, number_of, total, reach, skew):
    if number_of == 2:
        one = jax.random.randint(own_key, (), max(1, total - reach), min(reach, total - 1) + 1)
        return jnp.stack([one, total - one])
    sizes = jnp.asarray(length_profile(number_of, total, reach, skew), jnp.int32)
    twos = (number_of - 1) // 2
    donor, sink = sizes[1:1 + 2 * twos:2], sizes[2:2 + 2 * twos:2]
    slack = jnp.minimum(donor - 1, reach - sink)
    passed = jax.random.randint(jax.random.fold_in(own_key, 1), (twos,), 0, 1 << 20) % (slack + 1)
    sizes = sizes.at[1:1 + 2 * twos:2].set(donor - passed).at[2:2 + 2 * twos:2].set(sink + passed)
    return sizes[jax.random.permutation(jax.random.fold_in(own_key, 2), number_of)]


def centred(own_key, dims, scale, most, shards=(), held_as=jnp.bfloat16):
    values = scale * jax.random.normal(own_key, dims, jnp.float32)
    if shards:
        values = values * block_levels(own_key, dims, shards, -0.22, 0.18)
    return jnp.clip(values, -most, most).astype(held_as)


def setup_inputs(seed: int = 0) -> dict:
    seeds = jax.random.split(jax.random.key(seed), 8)
    return {
        "hidden": centred(seeds[0], (SEQ, D), 1.0, 6.0, ((0, 16), (1, 2))),
        "norm_gain": jnp.clip(1.0 + 0.1 * jax.random.normal(seeds[1], (D,), jnp.float32), 0.5, 1.5),
        "w_query": draw_w_query(jax.random.fold_in(seeds[7], 71), 0),
        "w_key": draw_w_key(jax.random.fold_in(seeds[7], 71), 0),
        "w_value": centred(seeds[4], (D, KV_HEADS * HEAD_SIZE), D ** -0.5, 0.09375, ((1, 2),)),
        "w_out": centred(seeds[5], (HEADS * HEAD_SIZE, D), (HEADS * HEAD_SIZE // 32) ** -0.5, 0.5, ((0, 2),)),
        "doc_ids": jnp.searchsorted(jnp.cumsum(uneven(seeds[6], DOCS, SEQ, LONGEST, 2)), jnp.arange(SEQ), side="right").astype(jnp.int32),
    }


epsilon = 1e-05
rope_base = 500000.0

def rotate(vectors, positions):
    half = HEAD_SIZE // 2
    freqs = rope_base ** (-jnp.arange(half, dtype=jnp.float32) * 2.0 / HEAD_SIZE)
    angles = positions.astype(jnp.float32)[:, None] * freqs[None, :]
    cosine = jnp.cos(angles)[:, None, :]
    sine = jnp.sin(angles)[:, None, :]
    first = vectors[..., :half]
    second = vectors[..., half:]
    return jnp.concatenate([first * cosine - second * sine, second * cosine + first * sine], axis=-1)

def attend_block(loop_state, query_matrix, query_pos, query_doc, key_matrix, value_matrix, key_pos, key_doc):
    best, total, running_output = loop_state
    logit_matrix = jnp.einsum('ucpm,ycm->cpuy', query_matrix.astype(jnp.float32), key_matrix.astype(jnp.float32)) * HEAD_SIZE ** (-0.5)
    allowed = (key_pos[None, :] <= query_pos[:, None]) & (key_doc[None, :] == query_doc[:, None])
    masked = jnp.where(allowed, logit_matrix, jnp.float32(-1e+30))
    new_best = jnp.maximum(best, lax.optimization_barrier(jnp.max(masked, axis=-1)))
    correction_scale = jnp.exp(best - new_best)
    attention_weights = jnp.where(allowed, jnp.exp(logit_matrix - new_best[..., None]), jnp.float32(0.0))
    total = total * correction_scale + lax.optimization_barrier(jnp.sum(attention_weights, axis=-1))
    rounded_weights = attention_weights.astype(jnp.bfloat16).astype(jnp.float32)
    running_output = running_output * correction_scale[..., None] + jnp.einsum('sfec,csh->sfeh', rounded_weights, value_matrix.astype(jnp.float32))
    return (new_best, total, running_output)

def reference(hidden, norm_gain, w_query, w_key, w_value, w_out, doc_ids):
    seq_len = hidden.shape[0]
    group = HEADS // KV_HEADS
    wide = hidden.astype(jnp.float32)
    inverse_rms = lax.rsqrt(lax.optimization_barrier(jnp.mean(wide * wide, axis=1, keepdims=True)) + epsilon)
    normed = (wide * inverse_rms * norm_gain.astype(jnp.float32)[None, :]).astype(jnp.bfloat16)
    positions = jnp.arange(seq_len, dtype=jnp.int32)
    query_raw = jnp.dot(normed, w_query, preferred_element_type=jnp.float32).reshape(seq_len, HEADS, HEAD_SIZE)
    key_raw = jnp.dot(normed, w_key, preferred_element_type=jnp.float32).reshape(seq_len, KV_HEADS, HEAD_SIZE)
    query_matrix = rotate(query_raw, positions).astype(jnp.bfloat16).reshape(seq_len, KV_HEADS, group, HEAD_SIZE)
    key_matrix = rotate(key_raw, positions).astype(jnp.bfloat16)
    value_matrix = jnp.dot(normed, w_value, preferred_element_type=jnp.float32).astype(jnp.bfloat16).reshape(seq_len, KV_HEADS, HEAD_SIZE)
    block_index = TOK_DEV if TOK_DEV <= 512 else 512
    blocks = seq_len // block_index

    def one_query_block(index):
        start = (index * block_index).astype(jnp.int32)
        query_blk = lax.dynamic_slice_in_dim(query_matrix, start, block_index, 0)
        query_pos = start + jnp.arange(block_index, dtype=jnp.int32)
        query_doc = lax.dynamic_slice_in_dim(doc_ids, start, block_index, 0)

        def loop_body(loop_state, key_block_index):
            key_offset = (key_block_index * block_index).astype(jnp.int32)

            def work(state):
                key_blk = lax.dynamic_slice_in_dim(key_matrix, key_offset, block_index, 0)
                value_blk = lax.dynamic_slice_in_dim(value_matrix, key_offset, block_index, 0)
                key_pos = key_offset + jnp.arange(block_index, dtype=jnp.int32)
                key_doc = lax.dynamic_slice_in_dim(doc_ids, key_offset, block_index, 0)
                return attend_block(state, query_blk, query_pos, query_doc, key_blk, value_blk, key_pos, key_doc)
            return (lax.cond(key_offset <= start + block_index - 1, work, lambda state: state, loop_state), None)
        init = (jnp.full((KV_HEADS, group, block_index), -1e+30, jnp.float32), jnp.zeros((KV_HEADS, group, block_index), jnp.float32), jnp.zeros((KV_HEADS, group, block_index, HEAD_SIZE), jnp.float32))
        final, _ = lax.scan(loop_body, init, jnp.arange(blocks, dtype=jnp.int32))
        result = final[2] / final[1][..., None]
        return jnp.transpose(result, (2, 0, 1, 3)).reshape(block_index, HEADS * HEAD_SIZE).astype(jnp.bfloat16)
    attended = lax.map(one_query_block, jnp.arange(blocks, dtype=jnp.int32)).reshape(seq_len, HEADS * HEAD_SIZE)
    width_cols = HEADS * HEAD_SIZE // N_TP
    mixed = jnp.zeros((seq_len, hidden.shape[1]), jnp.float32)
    for group_index in range(N_TP):
        lower = group_index * width_cols
        partial_sum = jnp.dot(attended[:, lower:lower + width_cols], w_out[lower:lower + width_cols], preferred_element_type=jnp.float32).astype(jnp.bfloat16)
        partial_sum = lax.optimization_barrier(partial_sum)
        mixed = mixed + partial_sum.astype(jnp.float32)
    return mixed.astype(jnp.bfloat16)
```

```python
import functools

import jax
import jax.numpy as jnp
from jax import lax
from jax.experimental import pallas as pl
from jax.experimental.pallas import tpu as pltpu
from jax.sharding import PartitionSpec as P


HEAD_SIZE = 128

epsilon = 1e-05
rope_base = 500000.0
MASKED = -1e30
LOG2E = 1.4426950408889634
PLANE = 4
VMEM = 32 * 1024 * 1024
GRANT = 24 * 1024 * 1024


def turn(vectors, cosine, sine):
    heads = [
        vectors[:, low : low + HEAD_SIZE] for low in range(0, vectors.shape[1], HEAD_SIZE)
    ]
    return [
        (head * cosine + pltpu.roll(head, HEAD_SIZE // 2, 1) * sine).astype(jnp.bfloat16)
        for head in heads
    ]


def key_value_kernel(n_tp, block, info, *refs):
    pieces, refs = refs[:n_tp], refs[n_tp:]
    gain_ref, cos_ref, sin_ref, key_hbm, value_hbm, out_ref, normed_hbm = refs[:7]
    held, normed_ref, key_ref, value_ref, piece_sem, weight_sem, out_sem = refs[7:]
    tokens, features = pieces[0].shape
    width = features * n_tp
    steps = key_hbm.shape[1] // block
    piece_copies = [
        pltpu.make_async_copy(piece, held.at[i], piece_sem.at[i]) for i, piece in enumerate(pieces)
    ]
    for copy in piece_copies:
        copy.start()
    weight_copies = []
    for step in range(steps):
        columns = pl.ds(step * block, block)
        for at, (source, target) in enumerate(((key_hbm, key_ref), (value_hbm, value_ref))):
            copy = pltpu.make_async_copy(
                source.at[:, columns], target.at[step], weight_sem.at[2 * step + at]
            )
            copy.start()
            weight_copies.append(copy)
    total = None
    for i, copy in enumerate(piece_copies):
        copy.wait()
        wide = held[i].astype(jnp.float32)
        squares = jnp.sum(wide * wide, axis=1, keepdims=True)
        total = squares if total is None else total + squares
    scale = lax.rsqrt(total / width + epsilon)
    for i in range(n_tp):
        owner = lax.rem(info[10] - i + n_tp, n_tp)
        columns = pl.ds(pl.multiple_of(owner * features, HEAD_SIZE), features)
        normed_ref[:, columns] = (
            held[i].astype(jnp.float32) * scale * gain_ref[0:1, columns]
        ).astype(jnp.bfloat16)
    normed_copy = pltpu.make_async_copy(normed_ref, normed_hbm, out_sem)
    normed_copy.start()
    heads = block // HEAD_SIZE
    for step in range(steps):
        weight_copies[2 * step].wait()
        keys = jnp.dot(normed_ref[...], key_ref[step], preferred_element_type=jnp.float32)
        turned = turn(keys, cos_ref[...], sin_ref[...])
        weight_copies[2 * step + 1].wait()
        values = jnp.dot(normed_ref[...], value_ref[step], preferred_element_type=jnp.float32)
        for head in range(heads):
            out_ref[step * heads + head, :, :HEAD_SIZE] = turned[head]
            mine = values[:, head * HEAD_SIZE : (head + 1) * HEAD_SIZE]
            for low in range(0, tokens, HEAD_SIZE):
                out_ref[step * heads + head, low : low + HEAD_SIZE, HEAD_SIZE:] = mine[
                    low : low + HEAD_SIZE, :
                ].T.astype(jnp.bfloat16)
    normed_copy.wait()


def project_keys(info, pieces, gain, cosine, sine, w_key, w_value):
    n_tp = len(pieces)
    tokens, features = pieces[0].shape
    depth, columns = w_key.shape
    block = min(2 * HEAD_SIZE, columns)
    steps = columns // block
    away = pl.BlockSpec(memory_space=pl.ANY)
    near = pl.BlockSpec(memory_space=pltpu.VMEM)
    return pl.pallas_call(
        functools.partial(key_value_kernel, n_tp, block),
        in_specs=[pl.BlockSpec(memory_space=pltpu.SMEM)]
        + [away] * n_tp
        + [near, near, near, away, away],
        out_specs=[near, away],
        out_shape=[
            jax.ShapeDtypeStruct((columns // HEAD_SIZE, tokens, 2 * HEAD_SIZE), jnp.bfloat16),
            jax.ShapeDtypeStruct((tokens, depth), jnp.bfloat16),
        ],
        scratch_shapes=[
            pltpu.VMEM((n_tp, tokens, features), jnp.bfloat16),
            pltpu.VMEM((tokens, depth), jnp.bfloat16),
            pltpu.VMEM((steps, depth, block), jnp.bfloat16),
            pltpu.VMEM((steps, depth, block), jnp.bfloat16),
            pltpu.SemaphoreType.DMA((n_tp,)),
            pltpu.SemaphoreType.DMA((2 * steps,)),
            pltpu.SemaphoreType.DMA,
        ],
        compiler_params=pltpu.CompilerParams(vmem_limit_bytes=VMEM),
        cost_estimate=pl.CostEstimate(
            flops=4 * tokens * depth * columns, bytes_accessed=4 * depth * columns, transcendentals=0
        ),
        name="project_keys",
    )(info, *pieces, gain, cosine, sine, w_key, w_value)


def product_kernel(block, rotary, offset, *refs):
    if rotary:
        cos_ref, sin_ref, refs = refs[0], refs[1], refs[2:]
    x_hbm, weight_hbm, out_ref, x_ref, held, x_sem, weight_sem = refs
    steps = out_ref.shape[1] // block

    def copy(step):
        columns = pl.ds(pl.multiple_of(offset[0] + step * block, HEAD_SIZE), block)
        return pltpu.make_async_copy(
            weight_hbm.at[:, columns], held.at[step], weight_sem.at[step]
        )

    x_copy = pltpu.make_async_copy(x_hbm, x_ref, x_sem)
    x_copy.start()
    for step in range(steps):
        copy(step).start()
    x_copy.wait()

    def body(step, _):
        copy(step).wait()
        result = jnp.dot(x_ref[...], held[step], preferred_element_type=jnp.float32)
        columns = pl.ds(pl.multiple_of(step * block, block), block)
        if rotary:
            result = jnp.concatenate(turn(result, cos_ref[...], sin_ref[...]), axis=1)
        out_ref[:, columns] = result.astype(jnp.bfloat16)
        return 0

    lax.fori_loop(0, steps, body, 0)


def product(x, weights, offset, columns, turns=None):
    tokens, depth = x.shape
    block = min(4 * HEAD_SIZE, columns)
    steps = columns // block
    away = pl.BlockSpec(memory_space=pl.ANY)
    near = pl.BlockSpec(memory_space=pltpu.VMEM)
    turns = turns or ()
    return pl.pallas_call(
        functools.partial(product_kernel, block, bool(turns)),
        in_specs=[pl.BlockSpec(memory_space=pltpu.SMEM)] + [near] * len(turns) + [away, away],
        out_specs=near,
        out_shape=jax.ShapeDtypeStruct((tokens, columns), jnp.bfloat16),
        scratch_shapes=[
            pltpu.VMEM((tokens, depth), jnp.bfloat16),
            pltpu.VMEM((steps, depth, block), jnp.bfloat16),
            pltpu.SemaphoreType.DMA,
            pltpu.SemaphoreType.DMA((steps,)),
        ],
        compiler_params=pltpu.CompilerParams(vmem_limit_bytes=VMEM),
        cost_estimate=pl.CostEstimate(
            flops=2 * tokens * depth * columns,
            bytes_accessed=2 * depth * columns,
            transcendentals=0,
        ),
        name="project_queries" if turns else "partial_product",
    )(offset, *turns, x, weights)


def attend_kernel(group, backs, part, first, last, info, start_ref, q_ref, *refs):
    sets, refs = refs[: 2 * len(backs)], refs[2 * len(backs) :]
    if not first:
        acc_in, stat_in, refs = refs[0], refs[1], refs[2:]
    if last:
        out_ref, refs = refs[0], refs[1:]
    acc, stat, rows, key_rows, value_cols, bias, score_a, score_b, units = refs
    scale = HEAD_SIZE**-0.5 * LOG2E
    queries = q_ref.shape[0]
    size = sets[0].shape[0] * sets[0].shape[2] // 2
    tiles = group // 2
    base, low_start, high_start = info[0], info[1 + 2 * part], info[2 + 2 * part]
    layer, inner = info[8], info[9]
    query_low = base + part * queries
    query_high = query_low + queries - 1

    if first:
        acc[...] = jnp.zeros(acc.shape, jnp.float32)
        stat[0, :tiles, :] = jnp.full((tiles, 2 * queries), MASKED, jnp.float32)
        stat[0, tiles:, :] = jnp.zeros((tiles, 2 * queries), jnp.float32)
    else:
        acc[...] = acc_in[...]
        stat[...] = stat_in[...]
    for tile in range(tiles):
        for side in range(2):
            head = 2 * tile + side
            rows[tile, side * queries : (side + 1) * queries, :] = q_ref[
                :, head * HEAD_SIZE : (head + 1) * HEAD_SIZE
            ]

    plain_count, masked_count = jnp.int32(0), jnp.int32(0)
    for at, back in enumerate(backs):
        for array in range(2):
            for half in range(2):
                unit = 4 * at + 2 * array + half
                block = (layer - back) * PLANE + (inner ^ (array + 2 * half))
                key_low = block * size
                key_high = key_low + size - 1
                need = (layer >= back) & (key_low <= query_high) & (key_high >= low_start)
                plain = need & (key_high <= query_low) & (key_low >= high_start)
                units[0, plain_count] = unit
                plain_count = plain_count + plain.astype(jnp.int32)
                units[1, masked_count] = unit
                units[2, masked_count] = key_low
                masked_count = masked_count + (need & ~plain).astype(jnp.int32)

                @pl.when(need)
                def _():
                    source = sets[2 * at + array]
                    piece = source.shape[2]
                    for i in range(size // piece):
                        entry = half * (size // piece) + i
                        key_rows[unit, i * piece : (i + 1) * piece, :] = source[
                            entry, 0, :, :HEAD_SIZE
                        ]
                        for low in range(0, piece, HEAD_SIZE):
                            at_token = i * piece + low
                            value_cols[unit, :, at_token : at_token + HEAD_SIZE] = source[
                                entry, 0, low : low + HEAD_SIZE, HEAD_SIZE:
                            ]

    @pl.when(pl.program_id(0) == 0)
    def _():
        def fill(index, _):
            shape = (size, queries)
            key_at = units[2, index] + lax.broadcasted_iota(jnp.int32, shape, 0)
            query_at = query_low + lax.broadcasted_iota(jnp.int32, shape, 1)
            allowed = (key_at >= start_ref[0:1, :]) & (key_at <= query_at)
            bias[index] = jnp.where(allowed, 0.0, MASKED)
            return 0

        lax.fori_loop(0, masked_count, fill, 0)

    def sweep(which, count, masked):
        def scores(index, tile, buffer):
            s = lax.dot_general(
                key_rows[units[which, index]],
                rows[tile],
                (((1,), (1,)), ((), ())),
                preferred_element_type=jnp.float32,
            )
            if masked:
                once = bias[index]
                s = s + jnp.concatenate([once, once], axis=1)
            buffer[...] = s
            return jnp.max(s, axis=0, keepdims=True)

        def weigh(index, tile, buffer, peak):
            old = stat[0, tile : tile + 1, :]
            new = jnp.maximum(old, peak)
            shrink = jnp.exp2((old - new) * scale)
            weights = jnp.exp2((buffer[...] - new) * scale)
            added = jnp.dot(
                value_cols[units[which, index]],
                weights.astype(jnp.bfloat16),
                preferred_element_type=jnp.float32,
            )
            acc[0, tile] = acc[0, tile] * shrink + added
            total = stat[0, tiles + tile : tiles + tile + 1, :]
            stat[0, tiles + tile : tiles + tile + 1, :] = total * shrink + jnp.sum(
                weights, axis=0, keepdims=True
            )
            stat[0, tile : tile + 1, :] = new

        def step(index, peak):
            following = jnp.minimum(index + 1, count - 1)
            for tile in range(0, tiles, 2):
                peak_b = scores(index, tile + 1, score_b)
                weigh(index, tile, score_a, peak)
                if tile + 2 < tiles:
                    peak = scores(index, tile + 2, score_a)
                else:
                    peak = scores(following, 0, score_a)
                weigh(index, tile + 1, score_b, peak_b)
            return peak

        @pl.when(count > 0)
        def _():
            lax.fori_loop(0, count, step, scores(0, 0, score_a))

    sweep(0, plain_count, False)
    sweep(1, masked_count, True)

    if last:
        for tile in range(tiles):
            done = acc[0, tile] / stat[0, tiles + tile : tiles + tile + 1, :]
            for side in range(2):
                head = 2 * tile + side
                out_ref[:, head * HEAD_SIZE : (head + 1) * HEAD_SIZE] = done[
                    :, side * queries : (side + 1) * queries
                ].T.astype(jnp.bfloat16)


def attend(info, start, queries, sets, backs, part, state, local_kv, last):
    tokens, columns = queries.shape
    group = columns // HEAD_SIZE // local_kv
    tiles = group // 2
    first = state is None
    arrays = [array for entry in sets for array in entry]
    entries, _, piece, _ = arrays[0].shape
    size = entries * piece // 2
    count = 2 * len(arrays)
    acc_shape = (1, tiles, HEAD_SIZE, 2 * tokens)
    stat_shape = (1, 2 * tiles, 2 * tokens)
    acc_block = pl.BlockSpec(acc_shape, lambda g, s: (g, 0, 0, 0))
    stat_block = pl.BlockSpec(stat_shape, lambda g, s: (g, 0, 0))
    q_block = pl.BlockSpec((tokens, group * HEAD_SIZE), lambda g, s: (0, g))
    in_specs = [pl.BlockSpec((8, tokens), lambda g, s: (0, part)), q_block]
    in_specs += [
        pl.BlockSpec((entries, 1, piece, 2 * HEAD_SIZE), lambda g, s: (0, g, 0, 0)) for _ in arrays
    ]
    operands = [info, start, queries, *arrays]
    scratch = [
        pltpu.VMEM((tiles, 2 * tokens, HEAD_SIZE), jnp.bfloat16),
        pltpu.VMEM((count, size, HEAD_SIZE), jnp.bfloat16),
        pltpu.VMEM((count, HEAD_SIZE, size), jnp.bfloat16),
        pltpu.VMEM((count, size, tokens), jnp.float32),
        pltpu.VMEM((size, 2 * tokens), jnp.float32),
        pltpu.VMEM((size, 2 * tokens), jnp.float32),
        pltpu.SMEM((3, count + 1), jnp.int32),
    ]
    aliases = {}
    if not first:
        in_specs += [acc_block, stat_block]
        operands += list(state)
        if not last:
            aliases = {len(operands) - 2: 0, len(operands) - 1: 1}
    if last:
        out_specs = [q_block]
        out_shape = [jax.ShapeDtypeStruct(queries.shape, jnp.bfloat16)]
        scratch = [
            pltpu.VMEM(acc_shape, jnp.float32),
            pltpu.VMEM(stat_shape, jnp.float32),
        ] + scratch
    else:
        out_specs = [acc_block, stat_block]
        out_shape = [
            jax.ShapeDtypeStruct((local_kv, *acc_shape[1:]), jnp.float32),
            jax.ShapeDtypeStruct((local_kv, *stat_shape[1:]), jnp.float32),
        ]
    return pl.pallas_call(
        functools.partial(attend_kernel, group, backs, part, first, last),
        grid_spec=pltpu.PrefetchScalarGridSpec(
            num_scalar_prefetch=1,
            grid=(local_kv,),
            in_specs=in_specs,
            out_specs=out_specs,
            scratch_shapes=scratch,
        ),
        out_shape=out_shape,
        input_output_aliases=aliases,
        compiler_params=pltpu.CompilerParams(
            dimension_semantics=("arbitrary",), vmem_limit_bytes=GRANT
        ),
        cost_estimate=pl.CostEstimate(
            flops=8 * columns * tokens * size * count,
            bytes_accessed=8 * 1024 * 1024,
            transcendentals=0,
        ),
        name="attend",
    )(*operands)


def set_groups(layers):
    return [(0,)] + ([(1, 2)] if layers > 2 else []) + [(back,) for back in range(3, layers)]


def sublayer(n_cp, n_tp, parts, hidden, norm_gain, w_query, w_key, w_value, w_out, doc_ids):
    tokens, features = hidden.shape
    local_kv = w_key.shape[1] // HEAD_SIZE
    layers = n_cp // PLANE
    piece = tokens // parts
    cp_rank = lax.axis_index("cp")
    tp_rank = lax.axis_index("tp")

    def tp_shift(array, shift):
        return lax.ppermute(array, "tp", [(i, (i + shift) % n_tp) for i in range(n_tp)])

    def cp_shift(array, shift):
        return lax.ppermute(array, "cp", [(i, i + shift) for i in range(n_cp - shift)])

    gathered = []
    for part in range(parts):
        mine = hidden[part * piece : (part + 1) * piece]
        gathered.append([mine] + [tp_shift(mine, shift) for shift in range(1, n_tp)])

    buckets = jnp.arange(128, dtype=jnp.int32)
    counts = jnp.sum((doc_ids[:, None] == buckets[None, :]).astype(jnp.int32), axis=0)
    running = counts
    reach = 1
    while reach < n_cp:
        running = running + cp_shift(running, reach)
        reach *= 2
    before = running - counts
    base = cp_rank * tokens
    earlier = jnp.sum((doc_ids[None, :] < doc_ids[:, None]).astype(jnp.int32), axis=1)
    carried = jnp.sum(jnp.where(buckets == doc_ids[0], before, 0))
    start = base + earlier - jnp.where(doc_ids == doc_ids[0], carried, 0)
    start_rows = jnp.broadcast_to(start[None, :], (8, tokens))
    ends = []
    for part in range(parts):
        ends += [start[part * piece], start[(part + 1) * piece - 1]]
    entries = [base, *ends] + [0] * (7 - len(ends))
    entries += [lax.div(cp_rank, PLANE), lax.rem(cp_rank, PLANE), tp_rank]
    slots = jnp.arange(16, dtype=jnp.int32)
    info = jnp.zeros((16,), jnp.int32)
    for slot, entry in enumerate(entries):
        info = jnp.where(slots == slot, entry, info)

    lanes = jnp.arange(HEAD_SIZE, dtype=jnp.int32)
    half = HEAD_SIZE // 2
    freqs = rope_base ** (-jnp.where(lanes < half, lanes, lanes - half) * 2.0 / HEAD_SIZE)
    positions = base + jnp.arange(tokens, dtype=jnp.int32)
    angles = positions.astype(jnp.float32)[:, None] * freqs[None, :]
    cosine = jnp.cos(angles)
    sine = jnp.where(lanes < half, -1.0, 1.0)[None, :] * jnp.sin(angles)
    gain = norm_gain[None, :]

    near = [[] for _ in range(layers)]
    far = [[] for _ in range(layers)]
    q_parts = []
    cross = [(i, i ^ 2) for i in range(n_cp)]
    own_cross = [(i, i ^ 2) for i in range(n_cp) if not i & 2]
    for part in range(parts):
        cut = slice(part * piece, (part + 1) * piece)
        block, normed = project_keys(
            info, gathered[part], gain, cosine[cut], sine[cut], w_key, w_value
        )
        for back in range(layers):
            if back == 0:
                here = block
            elif back <= 2:
                here = cp_shift(block, back * PLANE)
            else:
                here = cp_shift(near[back - 1][part], PLANE)
            near[back].append(here)
            far[back].append(lax.ppermute(here, "cp", cross if back else own_cross))
        q_parts.append(
            product(normed, w_query, info[15:], w_query.shape[1], (cosine[cut], sine[cut]))
        )
    sets = []
    swap = [(i, i ^ 1) for i in range(n_cp)]
    for back in range(layers):
        local = jnp.stack(near[back] + far[back])
        sets.append([local, lax.ppermute(local, "cp", swap)])

    states = [None] * parts
    for backs in set_groups(layers):
        for part in range(parts):
            states[part] = attend(
                info, start_rows, q_parts[part], [sets[back] for back in backs], backs, part,
                states[part], local_kv, backs[-1] == layers - 1,
            )

    outs = []
    for part in range(parts):
        attended = states[part][0]
        received = []
        for shift in range(1, n_tp):
            owner = lax.rem(info[10:11] + shift, n_tp)
            received.append(
                tp_shift(product(attended, w_out, owner * features, features), shift)
            )
        own = product(attended, w_out, info[10:11] * features, features)
        mixed = own.astype(jnp.float32)
        for other in received:
            mixed = mixed + other.astype(jnp.float32)
        outs.append(mixed.astype(jnp.bfloat16))
    return jnp.concatenate(outs, axis=0)


def solution(mesh):
    in_specs = (
        P("cp", "tp"),
        P(),
        P(None, "tp"),
        P(None, "tp"),
        P(None, "tp"),
        P("tp", None),
        P("cp"),
    )
    out_specs = P("cp", "tp")
    body = functools.partial(sublayer, mesh.shape["cp"], mesh.shape["tp"], 2)
    return jax.shard_map(body, mesh=mesh, in_specs=in_specs, out_specs=out_specs, check_vma=False)
```

```python
import functools

import jax
import jax.numpy as jnp
from jax import lax
from jax.experimental import pallas as pl
from jax.experimental.pallas import tpu as pltpu
from jax.sharding import PartitionSpec as P


HEAD_SIZE = 128

epsilon = 1e-05
rope_base = 500000.0
MASKED = -1e30
LOG2E = 1.4426950408889634
PLANE = 4
ALONE = 52 * 1024 * 1024
GRANT = 24 * 1024 * 1024


def turn(vectors, cosine, sine):
    heads = [
        vectors[:, low : low + HEAD_SIZE] for low in range(0, vectors.shape[1], HEAD_SIZE)
    ]
    return [
        (head * cosine + pltpu.roll(head, HEAD_SIZE // 2, 1) * sine).astype(jnp.bfloat16)
        for head in heads
    ]


def key_value_kernel(n_tp, block, info, *refs):
    pieces, refs = refs[:n_tp], refs[n_tp:]
    gain_ref, cos_ref, sin_ref, key_hbm, value_hbm, out_ref, normed_hbm = refs[:7]
    held, normed_ref, key_ref, value_ref, piece_sem, weight_sem, out_sem = refs[7:]
    tokens, features = pieces[0].shape
    width = features * n_tp
    steps = key_hbm.shape[1] // block
    piece_copies = [
        pltpu.make_async_copy(piece, held.at[i], piece_sem.at[i]) for i, piece in enumerate(pieces)
    ]
    for copy in piece_copies:
        copy.start()
    weight_copies = []
    for step in range(steps):
        columns = pl.ds(step * block, block)
        for at, (source, target) in enumerate(((key_hbm, key_ref), (value_hbm, value_ref))):
            copy = pltpu.make_async_copy(
                source.at[:, columns], target.at[step], weight_sem.at[2 * step + at]
            )
            copy.start()
            weight_copies.append(copy)
    total = None
    for i, copy in enumerate(piece_copies):
        copy.wait()
        wide = held[i].astype(jnp.float32)
        squares = jnp.sum(wide * wide, axis=1, keepdims=True)
        total = squares if total is None else total + squares
    scale = lax.rsqrt(total / width + epsilon)
    for i in range(n_tp):
        owner = lax.rem(info[10] - i + n_tp, n_tp)
        columns = pl.ds(pl.multiple_of(owner * features, HEAD_SIZE), features)
        normed_ref[:, columns] = (
            held[i].astype(jnp.float32) * scale * gain_ref[0:1, columns]
        ).astype(jnp.bfloat16)
    normed_copy = pltpu.make_async_copy(normed_ref, normed_hbm, out_sem)
    normed_copy.start()
    heads = block // HEAD_SIZE
    for step in range(steps):
        weight_copies[2 * step].wait()
        keys = jnp.dot(normed_ref[...], key_ref[step], preferred_element_type=jnp.float32)
        turned = turn(keys, cos_ref[...], sin_ref[...])
        weight_copies[2 * step + 1].wait()
        values = jnp.dot(normed_ref[...], value_ref[step], preferred_element_type=jnp.float32)
        for head in range(heads):
            out_ref[step * heads + head, :, :HEAD_SIZE] = turned[head]
            mine = values[:, head * HEAD_SIZE : (head + 1) * HEAD_SIZE]
            for low in range(0, tokens, HEAD_SIZE):
                out_ref[step * heads + head, low : low + HEAD_SIZE, HEAD_SIZE:] = mine[
                    low : low + HEAD_SIZE, :
                ].T.astype(jnp.bfloat16)
    normed_copy.wait()


def project_keys(info, pieces, gain, cosine, sine, w_key, w_value):
    n_tp = len(pieces)
    tokens, features = pieces[0].shape
    depth, columns = w_key.shape
    block = min(2 * HEAD_SIZE, columns)
    steps = columns // block
    away = pl.BlockSpec(memory_space=pltpu.HBM)
    near = pl.BlockSpec(memory_space=pltpu.VMEM)
    return pl.pallas_call(
        functools.partial(key_value_kernel, n_tp, block),
        in_specs=[pl.BlockSpec(memory_space=pltpu.SMEM)]
        + [away] * n_tp
        + [near, near, near, away, away],
        out_specs=[near, away],
        out_shape=[
            jax.ShapeDtypeStruct((columns // HEAD_SIZE, tokens, 2 * HEAD_SIZE), jnp.bfloat16),
            jax.ShapeDtypeStruct((tokens, depth), jnp.bfloat16),
        ],
        scratch_shapes=[
            pltpu.VMEM((n_tp, tokens, features), jnp.bfloat16),
            pltpu.VMEM((tokens, depth), jnp.bfloat16),
            pltpu.VMEM((steps, depth, block), jnp.bfloat16),
            pltpu.VMEM((steps, depth, block), jnp.bfloat16),
            pltpu.SemaphoreType.DMA((n_tp,)),
            pltpu.SemaphoreType.DMA((2 * steps,)),
            pltpu.SemaphoreType.DMA,
        ],
        compiler_params=pltpu.CompilerParams(vmem_limit_bytes=ALONE),
        cost_estimate=pl.CostEstimate(
            flops=4 * tokens * depth * columns, bytes_accessed=4 * depth * columns, transcendentals=0
        ),
        name="project_keys",
    )(info, *pieces, gain, cosine, sine, w_key, w_value)


def product_kernel(block, parts, rotary, offset, *refs):
    if rotary:
        cos_ref, sin_ref, refs = refs[0], refs[1], refs[2:]
    x_hbm, weight_hbm, out_refs = refs[:parts], refs[parts], refs[parts + 1 : 2 * parts + 1]
    x_ref, held, x_sem, weight_sem = refs[2 * parts + 1 :]
    rows = out_refs[0].shape[0]
    steps = out_refs[0].shape[1] // block

    def copy(step):
        columns = pl.ds(pl.multiple_of(offset[0] + step * block, HEAD_SIZE), block)
        return pltpu.make_async_copy(
            weight_hbm.at[:, columns], held.at[step], weight_sem.at[step]
        )

    x_copies = [
        pltpu.make_async_copy(x, x_ref.at[pl.ds(i * rows, rows)], x_sem.at[i])
        for i, x in enumerate(x_hbm)
    ]
    for x_copy in x_copies:
        x_copy.start()
    for step in range(steps):
        copy(step).start()
    for x_copy in x_copies:
        x_copy.wait()

    def body(step, _):
        copy(step).wait()
        result = jnp.dot(x_ref[...], held[step], preferred_element_type=jnp.float32)
        columns = pl.ds(pl.multiple_of(step * block, block), block)
        if rotary:
            result = jnp.concatenate(turn(result, cos_ref[...], sin_ref[...]), axis=1)
        result = result.astype(jnp.bfloat16)
        for i, out_ref in enumerate(out_refs):
            out_ref[:, columns] = result[i * rows : (i + 1) * rows]
        return 0

    lax.fori_loop(0, steps, body, 0)


def product(xs, weights, offset, columns, turns=()):
    rows, depth = xs[0].shape
    tokens = rows * len(xs)
    block = min(4 * HEAD_SIZE, columns)
    steps = columns // block
    away = pl.BlockSpec(memory_space=pltpu.HBM)
    near = pl.BlockSpec(memory_space=pltpu.VMEM)
    return pl.pallas_call(
        functools.partial(product_kernel, block, len(xs), bool(turns)),
        in_specs=[pl.BlockSpec(memory_space=pltpu.SMEM)]
        + [near] * len(turns)
        + [away] * (len(xs) + 1),
        out_specs=[near] * len(xs),
        out_shape=[jax.ShapeDtypeStruct((rows, columns), jnp.bfloat16)] * len(xs),
        scratch_shapes=[
            pltpu.VMEM((tokens, depth), jnp.bfloat16),
            pltpu.VMEM((steps, depth, block), jnp.bfloat16),
            pltpu.SemaphoreType.DMA((len(xs),)),
            pltpu.SemaphoreType.DMA((steps,)),
        ],
        compiler_params=pltpu.CompilerParams(vmem_limit_bytes=ALONE),
        cost_estimate=pl.CostEstimate(
            flops=2 * tokens * depth * columns,
            bytes_accessed=2 * depth * columns,
            transcendentals=0,
        ),
        name="project_queries" if turns else "partial_product",
    )(offset, *turns, *xs, weights)


def attend_kernel(group, backs, part, first, last, n_tp, info, start_ref, q_ref, *refs):
    sets, refs = refs[: 2 * len(backs)], refs[2 * len(backs) :]
    if not first:
        acc_in, stat_in, refs = refs[0], refs[1], refs[2:]
    if last:
        out_hbm, out_ref, product_refs, refs = refs[0], refs[1], refs[2 : n_tp + 1], refs[n_tp + 1 :]
        attended, held, weight_sem, refs = refs[0], refs[1], refs[2], refs[3:]
        steps, _, block = held.shape
        features = block * steps // (n_tp - 1) if n_tp > 1 else 0

        def weight_copy(step):
            shift = 1 + lax.div(step * block, features)
            owner = lax.rem(info[10] + shift, n_tp)
            low = owner * features + lax.rem(step * block, features)
            return pltpu.make_async_copy(
                out_hbm.at[:, pl.ds(pl.multiple_of(low, HEAD_SIZE), block)],
                held.at[step],
                weight_sem.at[step],
            )

        @pl.when(pl.program_id(0) == 0)
        def _():
            for step in range(steps):
                weight_copy(step).start()

    acc, stat, rows, key_rows, value_cols, bias, score_a, score_b, units = refs
    scale = HEAD_SIZE**-0.5 * LOG2E
    queries = q_ref.shape[0]
    size = sets[0].shape[0] * sets[0].shape[2] // 2
    tiles = group // 2
    base, low_start, high_start = info[0], info[1 + 2 * part], info[2 + 2 * part]
    layer, inner = info[8], info[9]
    query_low = base + part * queries
    query_high = query_low + queries - 1

    if first:
        acc[...] = jnp.zeros(acc.shape, jnp.float32)
        stat[0, :tiles, :] = jnp.full((tiles, 2 * queries), MASKED, jnp.float32)
        stat[0, tiles:, :] = jnp.zeros((tiles, 2 * queries), jnp.float32)
    else:
        acc[...] = acc_in[...]
        stat[...] = stat_in[...]
    for tile in range(tiles):
        for side in range(2):
            head = 2 * tile + side
            rows[tile, side * queries : (side + 1) * queries, :] = q_ref[
                :, head * HEAD_SIZE : (head + 1) * HEAD_SIZE
            ]

    plain_count, masked_count = jnp.int32(0), jnp.int32(0)
    for at, back in enumerate(backs):
        for array in range(2):
            for half in range(2):
                unit = 4 * at + 2 * array + half
                key_block = (layer - back) * PLANE + (inner ^ (array + 2 * half))
                key_low = key_block * size
                key_high = key_low + size - 1
                need = (layer >= back) & (key_low <= query_high) & (key_high >= low_start)
                plain = need & (key_high <= query_low) & (key_low >= high_start)
                units[0, plain_count] = unit
                plain_count = plain_count + plain.astype(jnp.int32)
                units[1, masked_count] = unit
                units[2, masked_count] = key_low
                masked_count = masked_count + (need & ~plain).astype(jnp.int32)

                @pl.when(need)
                def _():
                    source = sets[2 * at + array]
                    piece = source.shape[2]
                    for i in range(size // piece):
                        entry = half * (size // piece) + i
                        key_rows[unit, i * piece : (i + 1) * piece, :] = source[
                            entry, 0, :, :HEAD_SIZE
                        ]
                        for low in range(0, piece, HEAD_SIZE):
                            at_token = i * piece + low
                            value_cols[unit, :, at_token : at_token + HEAD_SIZE] = source[
                                entry, 0, low : low + HEAD_SIZE, HEAD_SIZE:
                            ]

    @pl.when(pl.program_id(0) == 0)
    def _():
        def fill(index, _):
            shape = (size, queries)
            key_at = units[2, index] + lax.broadcasted_iota(jnp.int32, shape, 0)
            query_at = query_low + lax.broadcasted_iota(jnp.int32, shape, 1)
            allowed = (key_at >= start_ref[0:1, :]) & (key_at <= query_at)
            bias[index] = jnp.where(allowed, 0.0, MASKED)
            return 0

        lax.fori_loop(0, masked_count, fill, 0)

    def sweep(which, count, masked):
        def scores(index, tile, buffer):
            s = lax.dot_general(
                key_rows[units[which, index]],
                rows[tile],
                (((1,), (1,)), ((), ())),
                preferred_element_type=jnp.float32,
            )
            if masked:
                once = bias[index]
                s = s + jnp.concatenate([once, once], axis=1)
            buffer[...] = s
            return jnp.max(s, axis=0, keepdims=True)

        def weigh(index, tile, buffer, peak):
            old = stat[0, tile : tile + 1, :]
            new = jnp.maximum(old, peak)
            shrink = jnp.exp2((old - new) * scale)
            weights = jnp.exp2((buffer[...] - new) * scale)
            added = jnp.dot(
                value_cols[units[which, index]],
                weights.astype(jnp.bfloat16),
                preferred_element_type=jnp.float32,
            )
            acc[0, tile] = acc[0, tile] * shrink + added
            total = stat[0, tiles + tile : tiles + tile + 1, :]
            stat[0, tiles + tile : tiles + tile + 1, :] = total * shrink + jnp.sum(
                weights, axis=0, keepdims=True
            )
            stat[0, tile : tile + 1, :] = new

        def step(index, peak):
            following = jnp.minimum(index + 1, count - 1)
            for tile in range(0, tiles, 2):
                peak_b = scores(index, tile + 1, score_b)
                weigh(index, tile, score_a, peak)
                if tile + 2 < tiles:
                    peak = scores(index, tile + 2, score_a)
                else:
                    peak = scores(following, 0, score_a)
                weigh(index, tile + 1, score_b, peak_b)
            return peak

        @pl.when(count > 0)
        def _():
            lax.fori_loop(0, count, step, scores(0, 0, score_a))

    sweep(0, plain_count, False)
    sweep(1, masked_count, True)

    if last:
        for tile in range(tiles):
            done = acc[0, tile] / stat[0, tiles + tile : tiles + tile + 1, :]
            for side in range(2):
                head = 2 * tile + side
                out_ref[:, head * HEAD_SIZE : (head + 1) * HEAD_SIZE] = done[
                    :, side * queries : (side + 1) * queries
                ].T.astype(jnp.bfloat16)
        width = group * HEAD_SIZE
        mine = pl.ds(pl.multiple_of(pl.program_id(0) * width, width), width)
        attended[:, mine] = out_ref[...]

        @pl.when(pl.program_id(0) == pl.num_programs(0) - 1)
        def _():
            each = steps // len(product_refs)
            for at, product_ref in enumerate(product_refs):

                def multiply(index, _):
                    step = at * each + index
                    weight_copy(step).wait()
                    columns = pl.ds(pl.multiple_of(index * block, block), block)
                    product_ref[:, columns] = jnp.dot(
                        attended[...], held[step], preferred_element_type=jnp.float32
                    ).astype(jnp.bfloat16)
                    return 0

                lax.fori_loop(0, each, multiply, 0)


def attend(info, start, queries, sets, backs, part, state, local_kv, w_out, n_tp):
    last = w_out is not None
    tokens, columns = queries.shape
    group = columns // HEAD_SIZE // local_kv
    tiles = group // 2
    first = state is None
    arrays = [array for entry in sets for array in entry]
    entries, _, piece, _ = arrays[0].shape
    size = entries * piece // 2
    count = 2 * len(arrays)
    acc_shape = (1, tiles, HEAD_SIZE, 2 * tokens)
    stat_shape = (1, 2 * tiles, 2 * tokens)
    acc_block = pl.BlockSpec(acc_shape, lambda g, s: (g, 0, 0, 0))
    stat_block = pl.BlockSpec(stat_shape, lambda g, s: (g, 0, 0))
    q_block = pl.BlockSpec((tokens, group * HEAD_SIZE), lambda g, s: (0, g))
    in_specs = [pl.BlockSpec((8, tokens), lambda g, s: (0, part)), q_block]
    in_specs += [
        pl.BlockSpec((entries, 1, piece, 2 * HEAD_SIZE), lambda g, s: (0, g, 0, 0)) for _ in arrays
    ]
    operands = [info, start, queries, *arrays]
    scratch = [
        pltpu.VMEM((tiles, 2 * tokens, HEAD_SIZE), jnp.bfloat16),
        pltpu.VMEM((count, size, HEAD_SIZE), jnp.bfloat16),
        pltpu.VMEM((count, HEAD_SIZE, size), jnp.bfloat16),
        pltpu.VMEM((count, size, tokens), jnp.float32),
        pltpu.VMEM((size, 2 * tokens), jnp.float32),
        pltpu.VMEM((size, 2 * tokens), jnp.float32),
        pltpu.SMEM((3, count + 1), jnp.int32),
    ]
    aliases = {}
    if not first:
        in_specs += [acc_block, stat_block]
        operands += list(state)
        if not last:
            aliases = {len(operands) - 2: 0, len(operands) - 1: 1}
    if last:
        depth, width = w_out.shape
        features = width // n_tp
        block = min(4 * HEAD_SIZE, features)
        steps = (n_tp - 1) * features // block
        in_specs += [pl.BlockSpec(memory_space=pltpu.HBM)]
        operands += [w_out]
        out_specs = [q_block] + [pl.BlockSpec((tokens, features), lambda g, s: (0, 0))] * (n_tp - 1)
        out_shape = [jax.ShapeDtypeStruct(queries.shape, jnp.bfloat16)]
        out_shape += [jax.ShapeDtypeStruct((tokens, features), jnp.bfloat16)] * (n_tp - 1)
        scratch = [
            pltpu.VMEM((tokens, depth), jnp.bfloat16),
            pltpu.VMEM((steps, depth, block), jnp.bfloat16),
            pltpu.SemaphoreType.DMA((steps,)),
            pltpu.VMEM(acc_shape, jnp.float32),
            pltpu.VMEM(stat_shape, jnp.float32),
        ] + scratch
    else:
        out_specs = [acc_block, stat_block]
        out_shape = [
            jax.ShapeDtypeStruct((local_kv, *acc_shape[1:]), jnp.float32),
            jax.ShapeDtypeStruct((local_kv, *stat_shape[1:]), jnp.float32),
        ]
    return pl.pallas_call(
        functools.partial(attend_kernel, group, backs, part, first, last, n_tp),
        grid_spec=pltpu.PrefetchScalarGridSpec(
            num_scalar_prefetch=1,
            grid=(local_kv,),
            in_specs=in_specs,
            out_specs=out_specs,
            scratch_shapes=scratch,
        ),
        out_shape=out_shape,
        input_output_aliases=aliases,
        compiler_params=pltpu.CompilerParams(
            dimension_semantics=("arbitrary",), vmem_limit_bytes=ALONE if last else GRANT
        ),
        cost_estimate=pl.CostEstimate(
            flops=8 * columns * tokens * size * count,
            bytes_accessed=8 * 1024 * 1024,
            transcendentals=0,
        ),
        name="attend",
    )(*operands)


def set_groups(layers):
    first = [(back,) for back in range(min(2, layers))]
    return first + [tuple(range(back, min(back + 2, layers))) for back in range(2, layers, 2)]


def sublayer(n_cp, n_tp, parts, hidden, norm_gain, w_query, w_key, w_value, w_out, doc_ids):
    tokens, features = hidden.shape
    local_kv = w_key.shape[1] // HEAD_SIZE
    layers = n_cp // PLANE
    piece = tokens // parts
    cp_rank = lax.axis_index("cp")
    tp_rank = lax.axis_index("tp")

    def tp_shift(array, shift):
        return lax.ppermute(array, "tp", [(i, (i + shift) % n_tp) for i in range(n_tp)])

    def cp_shift(array, shift):
        return lax.ppermute(array, "cp", [(i, i + shift) for i in range(n_cp - shift)])

    gathered = []
    for part in range(parts):
        mine = hidden[part * piece : (part + 1) * piece]
        gathered.append([mine] + [tp_shift(mine, shift) for shift in range(1, n_tp)])

    buckets = jnp.arange(128, dtype=jnp.int32)
    counts = jnp.sum((doc_ids[:, None] == buckets[None, :]).astype(jnp.int32), axis=0)
    running = counts
    reach = 1
    while reach < n_cp:
        running = running + cp_shift(running, reach)
        reach *= 2
    before = running - counts
    base = cp_rank * tokens
    earlier = jnp.sum((doc_ids[None, :] < doc_ids[:, None]).astype(jnp.int32), axis=1)
    carried = jnp.sum(jnp.where(buckets == doc_ids[0], before, 0))
    start = base + earlier - jnp.where(doc_ids == doc_ids[0], carried, 0)
    start_rows = jnp.broadcast_to(start[None, :], (8, tokens))
    ends = []
    for part in range(parts):
        ends += [start[part * piece], start[(part + 1) * piece - 1]]
    entries = [base, *ends] + [0] * (7 - len(ends))
    entries += [lax.div(cp_rank, PLANE), lax.rem(cp_rank, PLANE), tp_rank]
    slots = jnp.arange(16, dtype=jnp.int32)
    info = jnp.zeros((16,), jnp.int32)
    for slot, entry in enumerate(entries):
        info = jnp.where(slots == slot, entry, info)

    lanes = jnp.arange(HEAD_SIZE, dtype=jnp.int32)
    half = HEAD_SIZE // 2
    freqs = rope_base ** (-jnp.where(lanes < half, lanes, lanes - half) * 2.0 / HEAD_SIZE)
    positions = base + jnp.arange(tokens, dtype=jnp.int32)
    angles = positions.astype(jnp.float32)[:, None] * freqs[None, :]
    cosine = jnp.cos(angles)
    sine = jnp.where(lanes < half, -1.0, 1.0)[None, :] * jnp.sin(angles)
    gain = norm_gain[None, :]

    near = [[] for _ in range(layers)]
    far = [[] for _ in range(layers)]
    normed_parts = []
    cross = [(i, i ^ 2) for i in range(n_cp)]
    own_cross = [(i, i ^ 2) for i in range(n_cp) if not i & 2]
    for part in range(parts):
        cut = slice(part * piece, (part + 1) * piece)
        block, normed = project_keys(
            info, gathered[part], gain, cosine[cut], sine[cut], w_key, w_value
        )
        for back in range(layers):
            if back == 0:
                here = block
            else:
                here = cp_shift(near[back - 1][part], PLANE)
            near[back].append(here)
            far[back].append(lax.ppermute(here, "cp", cross if back else own_cross))
        normed_parts.append(normed)
    q_parts = product(normed_parts, w_query, info[15:], w_query.shape[1], (cosine, sine))
    sets = []
    swap = [(i, i ^ 1) for i in range(n_cp)]
    for back in range(layers):
        local = jnp.stack(near[back] + far[back])
        sets.append([local, lax.ppermute(local, "cp", swap)])

    states = [None] * parts
    for backs in set_groups(layers):
        for part in range(parts):
            states[part] = attend(
                info, start_rows, q_parts[part], [sets[back] for back in backs], backs, part,
                states[part], local_kv, w_out if backs[-1] == layers - 1 else None, n_tp,
            )

    outs = []
    for part in range(parts):
        attended, *partials = states[part]
        received = [tp_shift(partial, shift + 1) for shift, partial in enumerate(partials)]
        own = product([attended], w_out, info[10:11] * features, features)[0]
        mixed = own.astype(jnp.float32)
        for other in received:
            mixed = mixed + other.astype(jnp.float32)
        outs.append(mixed.astype(jnp.bfloat16))
    return jnp.concatenate(outs, axis=0)


def solution(mesh):
    in_specs = (
        P("cp", "tp"),
        P(),
        P(None, "tp"),
        P(None, "tp"),
        P(None, "tp"),
        P("tp", None),
        P("cp"),
    )
    out_specs = P("cp", "tp")
    body = functools.partial(sublayer, mesh.shape["cp"], mesh.shape["tp"], 2)
    return jax.shard_map(body, mesh=mesh, in_specs=in_specs, out_specs=out_specs, check_vma=False)
```

```python
import functools

import jax
import jax.numpy as jnp
from jax import lax
from jax.experimental import pallas as pl
from jax.experimental.pallas import tpu as pltpu
from jax.sharding import PartitionSpec as P


HEAD_SIZE = 128

epsilon = 1e-05
rope_base = 500000.0
MASKED = -1e30
LOG2E = 1.4426950408889634
PLANE = 4
ALONE = 49 * 1024 * 1024
GRANT = 24 * 1024 * 1024
LAST = 42 * 1024 * 1024


def turn(vectors, cosine, sine):
    heads = [
        vectors[:, low : low + HEAD_SIZE] for low in range(0, vectors.shape[1], HEAD_SIZE)
    ]
    return [
        (head * cosine + pltpu.roll(head, HEAD_SIZE // 2, 1) * sine).astype(jnp.bfloat16)
        for head in heads
    ]


def key_value_kernel(n_tp, block, info, *refs):
    pieces, refs = refs[:n_tp], refs[n_tp:]
    gain_ref, cos_ref, sin_ref, key_hbm, value_hbm, out_ref, normed_hbm = refs[:7]
    held, normed_ref, key_ref, value_ref, piece_sem, weight_sem, out_sem = refs[7:]
    tokens, features = pieces[0].shape
    width = features * n_tp
    steps = key_hbm.shape[1] // block
    piece_copies = [
        pltpu.make_async_copy(piece, held.at[i], piece_sem.at[i]) for i, piece in enumerate(pieces)
    ]
    for copy in piece_copies:
        copy.start()
    weight_copies = []
    for step in range(steps):
        columns = pl.ds(step * block, block)
        for at, (source, target) in enumerate(((key_hbm, key_ref), (value_hbm, value_ref))):
            copy = pltpu.make_async_copy(
                source.at[:, columns], target.at[step], weight_sem.at[2 * step + at]
            )
            copy.start()
            weight_copies.append(copy)
    total = None
    for i, copy in enumerate(piece_copies):
        copy.wait()
        wide = held[i].astype(jnp.float32)
        squares = jnp.sum(wide * wide, axis=1, keepdims=True)
        total = squares if total is None else total + squares
    scale = lax.rsqrt(total / width + epsilon)
    for i in range(n_tp):
        owner = lax.rem(info[10] - i + n_tp, n_tp)
        columns = pl.ds(pl.multiple_of(owner * features, HEAD_SIZE), features)
        normed_ref[:, columns] = (
            held[i].astype(jnp.float32) * scale * gain_ref[0:1, columns]
        ).astype(jnp.bfloat16)
    normed_copy = pltpu.make_async_copy(normed_ref, normed_hbm, out_sem)
    normed_copy.start()
    heads = block // HEAD_SIZE
    for step in range(steps):
        weight_copies[2 * step].wait()
        keys = jnp.dot(normed_ref[...], key_ref[step], preferred_element_type=jnp.float32)
        turned = turn(keys, cos_ref[...], sin_ref[...])
        weight_copies[2 * step + 1].wait()
        values = jnp.dot(normed_ref[...], value_ref[step], preferred_element_type=jnp.float32)
        for head in range(heads):
            out_ref[step * heads + head, :, :HEAD_SIZE] = turned[head]
            mine = values[:, head * HEAD_SIZE : (head + 1) * HEAD_SIZE]
            for low in range(0, tokens, HEAD_SIZE):
                out_ref[step * heads + head, low : low + HEAD_SIZE, HEAD_SIZE:] = mine[
                    low : low + HEAD_SIZE, :
                ].T.astype(jnp.bfloat16)
    normed_copy.wait()


def project_keys(info, pieces, gain, cosine, sine, w_key, w_value):
    n_tp = len(pieces)
    tokens, features = pieces[0].shape
    depth, columns = w_key.shape
    block = min(2 * HEAD_SIZE, columns)
    steps = columns // block
    away = pl.BlockSpec(memory_space=pltpu.HBM)
    near = pl.BlockSpec(memory_space=pltpu.VMEM)
    return pl.pallas_call(
        functools.partial(key_value_kernel, n_tp, block),
        in_specs=[pl.BlockSpec(memory_space=pltpu.SMEM)]
        + [away] * n_tp
        + [near, near, near, away, away],
        out_specs=[near, away],
        out_shape=[
            jax.ShapeDtypeStruct((columns // HEAD_SIZE, tokens, 2 * HEAD_SIZE), jnp.bfloat16),
            jax.ShapeDtypeStruct((tokens, depth), jnp.bfloat16),
        ],
        scratch_shapes=[
            pltpu.VMEM((n_tp, tokens, features), jnp.bfloat16),
            pltpu.VMEM((tokens, depth), jnp.bfloat16),
            pltpu.VMEM((steps, depth, block), jnp.bfloat16),
            pltpu.VMEM((steps, depth, block), jnp.bfloat16),
            pltpu.SemaphoreType.DMA((n_tp,)),
            pltpu.SemaphoreType.DMA((2 * steps,)),
            pltpu.SemaphoreType.DMA,
        ],
        compiler_params=pltpu.CompilerParams(vmem_limit_bytes=ALONE),
        cost_estimate=pl.CostEstimate(
            flops=4 * tokens * depth * columns, bytes_accessed=4 * depth * columns, transcendentals=0
        ),
        name="project_keys",
    )(info, *pieces, gain, cosine, sine, w_key, w_value)


def product_kernel(block, parts, rotary, offset, *refs):
    if rotary:
        cos_ref, sin_ref, refs = refs[0], refs[1], refs[2:]
    x_hbm, weight_hbm, out_refs = refs[:parts], refs[parts], refs[parts + 1 : 2 * parts + 1]
    x_ref, held, x_sem, weight_sem = refs[2 * parts + 1 :]
    rows = out_refs[0].shape[0]
    steps = out_refs[0].shape[1] // block

    def copy(step):
        columns = pl.ds(pl.multiple_of(offset[0] + step * block, HEAD_SIZE), block)
        return pltpu.make_async_copy(
            weight_hbm.at[:, columns], held.at[step], weight_sem.at[step]
        )

    x_copies = [
        pltpu.make_async_copy(x, x_ref.at[pl.ds(i * rows, rows)], x_sem.at[i])
        for i, x in enumerate(x_hbm)
    ]
    for x_copy in x_copies:
        x_copy.start()
    for step in range(steps):
        copy(step).start()
    for x_copy in x_copies:
        x_copy.wait()

    def body(step, _):
        copy(step).wait()
        result = jnp.dot(x_ref[...], held[step], preferred_element_type=jnp.float32)
        columns = pl.ds(pl.multiple_of(step * block, block), block)
        if rotary:
            result = jnp.concatenate(turn(result, cos_ref[...], sin_ref[...]), axis=1)
        result = result.astype(jnp.bfloat16)
        for i, out_ref in enumerate(out_refs):
            out_ref[:, columns] = result[i * rows : (i + 1) * rows]
        return 0

    lax.fori_loop(0, steps, body, 0)


def product(xs, weights, offset, columns, turns=()):
    rows, depth = xs[0].shape
    tokens = rows * len(xs)
    block = min(4 * HEAD_SIZE, columns)
    steps = columns // block
    away = pl.BlockSpec(memory_space=pltpu.HBM)
    near = pl.BlockSpec(memory_space=pltpu.VMEM)
    return pl.pallas_call(
        functools.partial(product_kernel, block, len(xs), bool(turns)),
        in_specs=[pl.BlockSpec(memory_space=pltpu.SMEM)]
        + [near] * len(turns)
        + [away] * (len(xs) + 1),
        out_specs=[near] * len(xs),
        out_shape=[jax.ShapeDtypeStruct((rows, columns), jnp.bfloat16)] * len(xs),
        scratch_shapes=[
            pltpu.VMEM((tokens, depth), jnp.bfloat16),
            pltpu.VMEM((steps, depth, block), jnp.bfloat16),
            pltpu.SemaphoreType.DMA((len(xs),)),
            pltpu.SemaphoreType.DMA((steps,)),
        ],
        compiler_params=pltpu.CompilerParams(vmem_limit_bytes=ALONE),
        cost_estimate=pl.CostEstimate(
            flops=2 * tokens * depth * columns,
            bytes_accessed=2 * depth * columns,
            transcendentals=0,
        ),
        name="project_queries" if turns else "partial_product",
    )(offset, *turns, *xs, weights)


def attend_kernel(group, backs, part, first, last, n_tp, info, start_ref, q_ref, *refs):
    sets, refs = refs[: 2 * len(backs)], refs[2 * len(backs) :]
    if not first:
        acc_in, stat_in, refs = refs[0], refs[1], refs[2:]
    if last:
        out_hbm, out_ref, product_refs, refs = refs[0], refs[1], refs[2 : n_tp + 1], refs[n_tp + 1 :]
        attended, held, weight_sem, refs = refs[0], refs[1], refs[2], refs[3:]
        steps, _, block = held.shape
        features = block * steps // (n_tp - 1) if n_tp > 1 else 0

        def weight_copy(step):
            shift = 1 + lax.div(step * block, features)
            owner = lax.rem(info[10] + shift, n_tp)
            low = owner * features + lax.rem(step * block, features)
            return pltpu.make_async_copy(
                out_hbm.at[:, pl.ds(pl.multiple_of(low, HEAD_SIZE), block)],
                held.at[step],
                weight_sem.at[step],
            )

        @pl.when(pl.program_id(0) == 0)
        def _():
            for step in range(steps):
                weight_copy(step).start()

    acc, stat, rows, key_rows, value_cols, bias, score_a, score_b, units = refs
    scale = HEAD_SIZE**-0.5 * LOG2E
    queries = q_ref.shape[0]
    size = sets[0].shape[0] * sets[0].shape[2] // 2
    tiles = group // 2
    base, low_start, high_start = info[0], info[1 + 2 * part], info[2 + 2 * part]
    layer, inner = info[8], info[9]
    query_low = base + part * queries
    query_high = query_low + queries - 1

    if first:
        acc[...] = jnp.zeros(acc.shape, jnp.float32)
        stat[0, :tiles, :] = jnp.full((tiles, 2 * queries), MASKED, jnp.float32)
        stat[0, tiles:, :] = jnp.zeros((tiles, 2 * queries), jnp.float32)
    else:
        acc[...] = acc_in[...]
        stat[...] = stat_in[...]
    for tile in range(tiles):
        for side in range(2):
            head = 2 * tile + side
            rows[tile, side * queries : (side + 1) * queries, :] = q_ref[
                :, head * HEAD_SIZE : (head + 1) * HEAD_SIZE
            ]

    plain_count, masked_count = jnp.int32(0), jnp.int32(0)
    for at, back in enumerate(backs):
        for array in range(2):
            for half in range(2):
                unit = 4 * at + 2 * array + half
                key_block = (layer - back) * PLANE + (inner ^ (array + 2 * half))
                key_low = key_block * size
                key_high = key_low + size - 1
                need = (layer >= back) & (key_low <= query_high) & (key_high >= low_start)
                plain = need & (key_high <= query_low) & (key_low >= high_start)
                units[0, plain_count] = unit
                plain_count = plain_count + plain.astype(jnp.int32)
                units[1, masked_count] = unit
                units[2, masked_count] = key_low
                masked_count = masked_count + (need & ~plain).astype(jnp.int32)

                @pl.when(need)
                def _():
                    source = sets[2 * at + array]
                    piece = source.shape[2]
                    for i in range(size // piece):
                        entry = half * (size // piece) + i
                        key_rows[unit, i * piece : (i + 1) * piece, :] = source[
                            entry, 0, :, :HEAD_SIZE
                        ]
                        for low in range(0, piece, HEAD_SIZE):
                            at_token = i * piece + low
                            value_cols[unit, :, at_token : at_token + HEAD_SIZE] = source[
                                entry, 0, low : low + HEAD_SIZE, HEAD_SIZE:
                            ]

    @pl.when(pl.program_id(0) == 0)
    def _():
        def fill(index, _):
            shape = (size, queries)
            key_at = units[2, index] + lax.broadcasted_iota(jnp.int32, shape, 0)
            query_at = query_low + lax.broadcasted_iota(jnp.int32, shape, 1)
            allowed = (key_at >= start_ref[0:1, :]) & (key_at <= query_at)
            bias[index] = jnp.where(allowed, 0.0, MASKED)
            return 0

        lax.fori_loop(0, masked_count, fill, 0)

    def sweep(which, count, masked):
        def scores(index, tile, buffer):
            s = lax.dot_general(
                key_rows[units[which, index]],
                rows[tile],
                (((1,), (1,)), ((), ())),
                preferred_element_type=jnp.float32,
            )
            if masked:
                once = bias[index]
                s = s + jnp.concatenate([once, once], axis=1)
            buffer[...] = s
            return jnp.max(s, axis=0, keepdims=True)

        def weigh(index, tile, buffer, peak):
            old = stat[0, tile : tile + 1, :]
            new = jnp.maximum(old, peak)
            shrink = jnp.exp2((old - new) * scale)
            weights = jnp.exp2((buffer[...] - new) * scale)
            added = jnp.dot(
                value_cols[units[which, index]],
                weights.astype(jnp.bfloat16),
                preferred_element_type=jnp.float32,
            )
            acc[0, tile] = acc[0, tile] * shrink + added
            total = stat[0, tiles + tile : tiles + tile + 1, :]
            stat[0, tiles + tile : tiles + tile + 1, :] = total * shrink + jnp.sum(
                weights, axis=0, keepdims=True
            )
            stat[0, tile : tile + 1, :] = new

        def step(index, peak):
            following = jnp.minimum(index + 1, count - 1)
            for tile in range(0, tiles, 2):
                peak_b = scores(index, tile + 1, score_b)
                weigh(index, tile, score_a, peak)
                if tile + 2 < tiles:
                    peak = scores(index, tile + 2, score_a)
                else:
                    peak = scores(following, 0, score_a)
                weigh(index, tile + 1, score_b, peak_b)
            return peak

        @pl.when(count > 0)
        def _():
            lax.fori_loop(0, count, step, scores(0, 0, score_a))

    sweep(0, plain_count, False)
    sweep(1, masked_count, True)

    if last:
        for tile in range(tiles):
            done = acc[0, tile] / stat[0, tiles + tile : tiles + tile + 1, :]
            for side in range(2):
                head = 2 * tile + side
                out_ref[:, head * HEAD_SIZE : (head + 1) * HEAD_SIZE] = done[
                    :, side * queries : (side + 1) * queries
                ].T.astype(jnp.bfloat16)
        width = group * HEAD_SIZE
        mine = pl.ds(pl.multiple_of(pl.program_id(0) * width, width), width)
        attended[:, mine] = out_ref[...]

        @pl.when(pl.program_id(0) == pl.num_programs(0) - 1)
        def _():
            each = steps // len(product_refs)
            for at, product_ref in enumerate(product_refs):

                def multiply(index, _):
                    step = at * each + index
                    weight_copy(step).wait()
                    columns = pl.ds(pl.multiple_of(index * block, block), block)
                    product_ref[:, columns] = jnp.dot(
                        attended[...], held[step], preferred_element_type=jnp.float32
                    ).astype(jnp.bfloat16)
                    return 0

                lax.fori_loop(0, each, multiply, 0)


def attend(info, start, queries, sets, backs, part, state, local_kv, w_out, n_tp):
    last = w_out is not None
    tokens, columns = queries.shape
    group = columns // HEAD_SIZE // local_kv
    tiles = group // 2
    first = state is None
    arrays = [array for entry in sets for array in entry]
    entries, _, piece, _ = arrays[0].shape
    size = entries * piece // 2
    count = 2 * len(arrays)
    acc_shape = (1, tiles, HEAD_SIZE, 2 * tokens)
    stat_shape = (1, 2 * tiles, 2 * tokens)
    acc_block = pl.BlockSpec(acc_shape, lambda g, s: (g, 0, 0, 0))
    stat_block = pl.BlockSpec(stat_shape, lambda g, s: (g, 0, 0))
    q_block = pl.BlockSpec((tokens, group * HEAD_SIZE), lambda g, s: (0, g))
    in_specs = [pl.BlockSpec((8, tokens), lambda g, s: (0, part)), q_block]
    in_specs += [
        pl.BlockSpec((entries, 1, piece, 2 * HEAD_SIZE), lambda g, s: (0, g, 0, 0)) for _ in arrays
    ]
    operands = [info, start, queries, *arrays]
    scratch = [
        pltpu.VMEM((tiles, 2 * tokens, HEAD_SIZE), jnp.bfloat16),
        pltpu.VMEM((count, size, HEAD_SIZE), jnp.bfloat16),
        pltpu.VMEM((count, HEAD_SIZE, size), jnp.bfloat16),
        pltpu.VMEM((count, size, tokens), jnp.float32),
        pltpu.VMEM((size, 2 * tokens), jnp.float32),
        pltpu.VMEM((size, 2 * tokens), jnp.float32),
        pltpu.SMEM((3, count + 1), jnp.int32),
    ]
    aliases = {}
    if not first:
        in_specs += [acc_block, stat_block]
        operands += list(state)
        if not last:
            aliases = {len(operands) - 2: 0, len(operands) - 1: 1}
    if last:
        depth, width = w_out.shape
        features = width // n_tp
        block = min(4 * HEAD_SIZE, features)
        steps = (n_tp - 1) * features // block
        in_specs += [pl.BlockSpec(memory_space=pltpu.HBM)]
        operands += [w_out]
        out_specs = [q_block] + [pl.BlockSpec((tokens, features), lambda g, s: (0, 0))] * (n_tp - 1)
        out_shape = [jax.ShapeDtypeStruct(queries.shape, jnp.bfloat16)]
        out_shape += [jax.ShapeDtypeStruct((tokens, features), jnp.bfloat16)] * (n_tp - 1)
        scratch = [
            pltpu.VMEM((tokens, depth), jnp.bfloat16),
            pltpu.VMEM((steps, depth, block), jnp.bfloat16),
            pltpu.SemaphoreType.DMA((steps,)),
            pltpu.VMEM(acc_shape, jnp.float32),
            pltpu.VMEM(stat_shape, jnp.float32),
        ] + scratch
    else:
        out_specs = [acc_block, stat_block]
        out_shape = [
            jax.ShapeDtypeStruct((local_kv, *acc_shape[1:]), jnp.float32),
            jax.ShapeDtypeStruct((local_kv, *stat_shape[1:]), jnp.float32),
        ]
    return pl.pallas_call(
        functools.partial(attend_kernel, group, backs, part, first, last, n_tp),
        grid_spec=pltpu.PrefetchScalarGridSpec(
            num_scalar_prefetch=1,
            grid=(local_kv,),
            in_specs=in_specs,
            out_specs=out_specs,
            scratch_shapes=scratch,
        ),
        out_shape=out_shape,
        input_output_aliases=aliases,
        compiler_params=pltpu.CompilerParams(
            dimension_semantics=("arbitrary",), vmem_limit_bytes=LAST if last else GRANT
        ),
        cost_estimate=pl.CostEstimate(
            flops=8 * columns * tokens * size * count,
            bytes_accessed=8 * 1024 * 1024,
            transcendentals=0,
        ),
        name="attend",
    )(*operands)


def set_groups(layers):
    first = [(back,) for back in range(min(2, layers))]
    return first + [tuple(range(back, min(back + 2, layers))) for back in range(2, layers, 2)]


def sublayer(n_cp, n_tp, parts, hidden, norm_gain, w_query, w_key, w_value, w_out, doc_ids):
    tokens, features = hidden.shape
    local_kv = w_key.shape[1] // HEAD_SIZE
    layers = n_cp // PLANE
    piece = tokens // parts
    cp_rank = lax.axis_index("cp")
    tp_rank = lax.axis_index("tp")
    tp_info = jnp.full((1,), tp_rank, jnp.int32)

    def tp_shift(array, shift):
        return lax.ppermute(array, "tp", [(i, (i + shift) % n_tp) for i in range(n_tp)])

    def cp_shift(array, shift):
        return lax.ppermute(array, "cp", [(i, i + shift) for i in range(n_cp - shift)])

    gathered = []
    for part in range(parts):
        mine = hidden[part * piece : (part + 1) * piece]
        gathered.append([mine] + [tp_shift(mine, shift) for shift in range(1, n_tp)])

    buckets = jnp.arange(128, dtype=jnp.int32)
    counts = jnp.sum((doc_ids[:, None] == buckets[None, :]).astype(jnp.int32), axis=0)
    running = counts
    reach = 1
    while reach < n_cp:
        further = [cp_shift(running, reach * times) for times in (1, 2, 3) if reach * times < n_cp]
        running = sum(further, running)
        reach *= 4
    before = running - counts
    base = cp_rank * tokens
    earlier = jnp.sum((doc_ids[None, :] < doc_ids[:, None]).astype(jnp.int32), axis=1)
    carried = jnp.sum(jnp.where(buckets == doc_ids[0], before, 0))
    start = base + earlier - jnp.where(doc_ids == doc_ids[0], carried, 0)
    start_rows = jnp.broadcast_to(start[None, :], (8, tokens))
    ends = []
    for part in range(parts):
        ends += [start[part * piece], start[(part + 1) * piece - 1]]
    entries = [base, *ends] + [0] * (7 - len(ends))
    entries += [lax.div(cp_rank, PLANE), lax.rem(cp_rank, PLANE), tp_rank]
    slots = jnp.arange(16, dtype=jnp.int32)
    info = jnp.zeros((16,), jnp.int32)
    for slot, entry in enumerate(entries):
        info = jnp.where(slots == slot, entry, info)

    lanes = jnp.arange(HEAD_SIZE, dtype=jnp.int32)
    half = HEAD_SIZE // 2
    freqs = rope_base ** (-jnp.where(lanes < half, lanes, lanes - half) * 2.0 / HEAD_SIZE)
    positions = base + jnp.arange(tokens, dtype=jnp.int32)
    angles = positions.astype(jnp.float32)[:, None] * freqs[None, :]
    cosine = jnp.cos(angles)
    sine = jnp.where(lanes < half, -1.0, 1.0)[None, :] * jnp.sin(angles)
    gain = norm_gain[None, :]

    near = [[] for _ in range(layers)]
    far = [[] for _ in range(layers)]
    normed_parts = []
    cross = [(i, i ^ 2) for i in range(n_cp)]
    own_cross = [(i, i ^ 2) for i in range(n_cp) if not i & 2]
    for part in range(parts):
        cut = slice(part * piece, (part + 1) * piece)
        block, normed = project_keys(
            info, gathered[part], gain, cosine[cut], sine[cut], w_key, w_value
        )
        for back in range(layers):
            if back == 0:
                here = block
            else:
                here = cp_shift(near[back - 1][part], PLANE)
            near[back].append(here)
            far[back].append(lax.ppermute(here, "cp", cross if back else own_cross))
        normed_parts.append(normed)
    q_parts = product(normed_parts, w_query, jnp.zeros((1,), jnp.int32), w_query.shape[1], (cosine, sine))
    sets = []
    swap = [(i, i ^ 1) for i in range(n_cp)]
    for back in range(layers):
        local = jnp.stack(near[back] + far[back])
        sets.append([local, lax.ppermute(local, "cp", swap)])

    states = [None] * parts
    for backs in set_groups(layers):
        for part in range(parts):
            states[part] = attend(
                info, start_rows, q_parts[part], [sets[back] for back in backs], backs, part,
                states[part], local_kv, w_out if backs[-1] == layers - 1 else None, n_tp,
            )

    outs = []
    for part in range(parts):
        attended, *partials = states[part]
        received = [tp_shift(partial, shift + 1) for shift, partial in enumerate(partials)]
        own = product([attended], w_out, tp_info * features, features)[0]
        mixed = own.astype(jnp.float32)
        for other in received:
            mixed = mixed + other.astype(jnp.float32)
        outs.append(mixed.astype(jnp.bfloat16))
    return jnp.concatenate(outs, axis=0)


def solution(mesh):
    in_specs = (
        P("cp", "tp"),
        P(),
        P(None, "tp"),
        P(None, "tp"),
        P(None, "tp"),
        P("tp", None),
        P("cp"),
    )
    out_specs = P("cp", "tp")
    body = functools.partial(sublayer, mesh.shape["cp"], mesh.shape["tp"], 2)
    return jax.shard_map(body, mesh=mesh, in_specs=in_specs, out_specs=out_specs, check_vma=False)
```
